32 devices in a mesh: blk: 16 (over z, y, core), mp: 2 (over x).
Axes of the slice: x: 2, y: 2, z: 4, core: 2. Of those that a mesh axis runs over, the one named last changes fastest.
Arguments:
- params: bfloat16 [16, 1024, 4096], P('blk', None, 'mp'), may hold values from -0.09375 to 0.09375
- hidden: bfloat16 [16, 384, 4096], P('blk', None, 'mp'), may hold values from -6 to 6
- targets: bfloat16 [16, 384, 1024], P('blk', None, 'mp'), may hold values from -6 to 6
Outputs:
- params_out: bfloat16 [16, 1024, 4096], P('blk', None, 'mp')
- errors: float32 [2], replicated
The draws below stay inside these ranges and needn't reach their ends.
All inputs are finite; a program needn't handle non-finite values.
Results may differ from the reference program's by a relative error of at most 0.0085.
Values may be sent and summed in bfloat16 or wider, within the bound.
A program may use at most 128 MiB of HBM per device.

```python
import jax
import jax.numpy as jnp
from jax import lax

D = 1024
TOK = 384
ITERS = 2
FF_WIN = 4096
REPL = 16


def steps_of(stream_key, dims, shards, least, top_value):
    level = 1.0
    for dim, parts in shards:
        steps = jax.random.uniform(jax.random.fold_in(jax.random.fold_in(stream_key, 6), dim), (parts,), jnp.float32, least / len(shards), top_value / len(shards))
        level = level * jnp.repeat(jnp.exp(steps), dims[dim] // parts).reshape((-1,) + (1,) * (len(dims) - 1 - dim))
    return level


def bell_draw(stream_key, shape, scale, most, cuts=(), kind=jnp.bfloat16):
    gain = steps_of(stream_key, shape, cuts, -0.22, 0.18) if cuts else 1.0
    array = jax.random.normal(stream_key, shape, jnp.float32) * scale * gain
    return jnp.minimum(jnp.maximum(array, -most), most).astype(kind)


def setup_inputs(seed: int = 0) -> dict:
    streams_of = jax.random.split(jax.random.key(seed), 4)
    return {
        "params": bell_draw(streams_of[0], (REPL, D, FF_WIN), FF_WIN ** -0.5, 0.09375, ((0, 16), (2, 2))),
        "hidden": bell_draw(streams_of[1], (REPL, TOK, FF_WIN), 1.0, 6.0, ((0, 16), (2, 2))),
        "targets": bell_draw(streams_of[2], (REPL, TOK, D), 1.0, 6.0, ((0, 16), (2, 2))),
    }


mix_third = 1.0 / 3.0
step_size = 0.1


def gradient(weight, hidden_one, targets_one):
    output = lax.dot_general(hidden_one, weight, (((1,), (1,)), ((), ())), preferred_element_type=jnp.float32)
    resid = (output - targets_one.astype(jnp.float32)).astype(jnp.bfloat16)
    grad = lax.dot_general(resid, hidden_one, (((0,), (0,)), ((), ())), preferred_element_type=jnp.float32)
    return grad / TOK


def one_item(item):
    return gradient(item[0], item[1], item[2])


def pick(stack, index):
    return lax.dynamic_index_in_dim(stack, (index % REPL).astype(jnp.int32), 0, keepdims=False).astype(jnp.float32)


def reference(params, hidden, targets):
    state = params
    older = lax.map(one_item, (params, hidden, targets))
    fresh = older
    track = older.astype(jnp.bfloat16)
    indices = jnp.arange(REPL, dtype=jnp.int32)
    err_list = []
    for step in range(ITERS):
        if step > 0:
            def track_row(index):
                blend = (pick(track, index - 1) + pick(track, index) + pick(track, index + 1)) * mix_third
                return (blend + pick(fresh, index) - pick(older, index)).astype(jnp.bfloat16)
            track = lax.map(track_row, indices)
            older = fresh

        def err_row(index):
            diff = pick(state, index) - pick(state, index + 1)
            return jnp.sum(diff * diff)
        err_list.append(jnp.sum(lax.map(err_row, indices)) / (FF_WIN * REPL))

        def state_row(index):
            blend = (pick(state, index - 1) + pick(state, index) + pick(state, index + 1)) * mix_third
            return (blend - step_size * pick(track, index)).astype(jnp.bfloat16)
        new_state = lax.map(state_row, indices)
        if step < ITERS - 1:
            fresh = lax.map(one_item, (new_state, hidden, targets))
        state = new_state
    return state, jnp.stack(err_list)
```

```python
import functools

import jax
import jax.numpy as jnp
from jax import lax
from jax.experimental import pallas as pl
from jax.experimental.pallas import tpu as pltpu
from jax.sharding import PartitionSpec as P

MESH = pl.DeviceIdType.MESH
CHUNKS = 4
COLS = 4
mix_third = 1.0 / 3.0
step_size = 0.1
F32 = jnp.float32
BF16 = jnp.bfloat16


def dot_nt(a, b):
    return lax.dot_general(a, b, (((1,), (1,)), ((), ())), preferred_element_type=F32)


def dot_nn(a, b):
    return lax.dot_general(a, b, (((1,), (0,)), ((), ())), preferred_element_type=F32)


def kernel(n, x, h, t, out, err, far, near, hn, rt, rt2, rn, ps, pr, acc, sems, one):
    d, wide = x.shape
    tokens = h.shape[0]
    half = t.shape[0]
    rows = d // CHUNKS
    cw = wide // COLS
    me = lax.axis_index("blk")
    mp = lax.axis_index("mp")
    core = lax.rem(me, 2)
    par = lax.rem(me // 2, 2)
    sib = me + 1 - 2 * core
    partner = me + 2 - 4 * par
    fwd_to = lax.rem(me + n + 4 - 8 * par, n)
    fwd_from = lax.rem(me + n - 4 + 8 * par, n)
    cross = lax.rem(me + n + 2 * core - 1, n)

    barrier = pltpu.get_barrier_semaphore()
    peers = [(sib, mp), (partner, mp), (fwd_to, mp), (fwd_from, mp), (cross, mp), (me, 1 - mp)]
    for peer in peers:
        pl.semaphore_signal(barrier, inc=1, device_id=peer, device_id_type=MESH)
    pl.semaphore_wait(barrier, len(peers))

    def rs(k):
        return pl.ds(k * rows, rows)

    def copy(src, dst, kind, k, dev):
        return pltpu.make_async_remote_copy(
            src_ref=src, dst_ref=dst, send_sem=sems.at[0, kind, k], recv_sem=sems.at[1, kind, k],
            device_id=dev, device_id_type=MESH)

    def c_own(k):
        return copy(x.at[rs(k)], far.at[par, rs(k)], 0, k, (partner, mp))

    def c_fwd(k):
        return copy(far.at[1 - par, rs(k)], far.at[par, rs(k)], 1, k, (fwd_to, mp))

    def c_cross(k):
        return copy(far.at[1 - core, rs(k)], near.at[1 - core, rs(k)], 2, k, (sib, mp))

    def c_rsib(k):
        return copy(rt.at[rs(k)], rn.at[core, rs(k)], 3, k, (sib, mp))

    def c_rcross(k):
        return copy(rt.at[rs(k)], rn.at[1 - core, rs(k)], 4, k, (cross, mp))

    def c_part(it, k):
        return copy(ps.at[it, rs(k)], pr.at[it, rs(k)], 5 + it, k, (me, 1 - mp))

    def c_hcross(j):
        cs = pl.ds(j * cw, cw)
        return copy(h.at[:, cs], hn.at[1 - core, :, cs], 7, j, (cross, mp))

    c_sib = pltpu.make_async_remote_copy(
        src_ref=x, dst_ref=near.at[core], send_sem=one.at[0, 0], recv_sem=one.at[1, 0],
        device_id=(sib, mp), device_id_type=MESH)
    c_hsib = pltpu.make_async_remote_copy(
        src_ref=h, dst_ref=hn.at[core], send_sem=one.at[0, 1], recv_sem=one.at[1, 1],
        device_id=(sib, mp), device_id_type=MESH)

    def send_part(it, k, value):
        first = k * rows
        mine = mp == first // half
        targ = t[pl.ds(first % half, rows), :].astype(F32)
        ps[it, rs(k), :] = (value - jnp.where(mine, targ, 0.0)).astype(BF16)
        c_part(it, k).start()

    def take_part(it, k, dst):
        c_part(it, k).wait_recv()
        dst[rs(k), :] = (ps[it, rs(k), :].astype(F32) + pr[it, rs(k), :].astype(F32)).astype(BF16)

    early = CHUNKS // 2
    for k in range(early):
        c_own(k).start()
    c_sib.start()
    c_hsib.start()
    acc[...] = jnp.zeros_like(acc)
    for k in range(CHUNKS):
        send_part(0, k, dot_nt(x[rs(k), :], h[...]))
    for k in range(CHUNKS):
        take_part(0, k, rt)
        c_rcross(k).start()
        c_rsib(k).start()
    for k in range(early, CHUNKS):
        c_own(k).start()
    for j in range(COLS):
        c_hcross(j).start()
    c_sib.wait_recv()

    for s in range(CHUNKS + 2):
        if s < CHUNKS:
            c_own(s).wait_recv()
            c_fwd(s).start()
        k = s - 1
        if 0 <= k < CHUNKS:
            c_fwd(k).wait_recv()
            c_cross(k).start()
            c_cross(k).wait_recv()

            def first_step(j, _, k=k):
                cs = pl.ds(pl.multiple_of(j * cw, cw), cw)
                track = (dot_nn(rt[rs(k), :], h[:, cs]) / tokens).astype(BF16)
                own = x[rs(k), cs].astype(F32)
                blend = (near[0, rs(k), cs].astype(F32) + own + near[1, rs(k), cs].astype(F32)) * mix_third
                out[rs(k), cs] = (blend - step_size * track.astype(F32)).astype(BF16)
                return 0

            lax.fori_loop(0, COLS, first_step, 0)
            send_part(1, k, dot_nt(out[rs(k), :], h[...]))
        k = s - 2
        if 0 <= k < CHUNKS:
            take_part(1, k, rt2)

    c_hsib.wait_recv()
    for k in range(CHUNKS):
        c_rsib(k).wait_recv()
        c_rcross(k).wait_recv()

    for j in range(COLS):
        c_hcross(j).wait_recv()
        cs = pl.ds(j * cw, cw)

        def last_step(k, _, cs=cs):
            r = pl.ds(pl.multiple_of(k * rows, rows), rows)
            older = dot_nn(rt[r, :], h[:, cs]) / tokens
            fresh = dot_nn(rt2[r, :], h[:, cs]) / tokens
            below = (dot_nn(rn[0, r, :], hn[0, :, cs]) / tokens).astype(BF16).astype(F32)
            above = (dot_nn(rn[1, r, :], hn[1, :, cs]) / tokens).astype(BF16).astype(F32)
            track = older.astype(BF16).astype(F32)
            track = ((below + track + above) * mix_third + fresh - older).astype(BF16).astype(F32)
            own = x[r, cs].astype(F32)
            lo = near[0, r, cs].astype(F32)
            hi = near[1, r, cs].astype(F32)
            x_lo = (far[0, r, cs].astype(F32) + lo + own) * mix_third - step_size * below
            x_hi = (own + hi + far[1, r, cs].astype(F32)) * mix_third - step_size * above
            x_lo = x_lo.astype(BF16).astype(F32)
            x_hi = x_hi.astype(BF16).astype(F32)
            x_me = out[r, cs].astype(F32)
            diff = own - hi
            acc[0:1, :] += jnp.sum(diff * diff, axis=0, keepdims=True)
            diff = x_me - x_hi
            acc[1:2, :] += jnp.sum(diff * diff, axis=0, keepdims=True)
            out[r, cs] = ((x_lo + x_me + x_hi) * mix_third - step_size * track).astype(BF16)
            return 0

        lax.fori_loop(0, CHUNKS, last_step, 0)

    err[...] = acc[...]
    c_sib.wait_send()
    c_hsib.wait_send()
    for k in range(CHUNKS):
        for c in (c_own(k), c_fwd(k), c_cross(k), c_rsib(k), c_rcross(k), c_part(0, k), c_part(1, k)):
            c.wait_send()
    for j in range(COLS):
        c_hcross(j).wait_send()


def solution(mesh):
    n = mesh.shape["blk"]

    def on_device(params, hidden, targets):
        x, h, t = params[0], hidden[0], targets[0].T
        d, wide = x.shape
        tokens = h.shape[0]
        total = wide * mesh.shape["mp"] * n
        vmem = pl.BlockSpec(memory_space=pltpu.VMEM)
        kinds = 8
        most = max(CHUNKS, COLS)
        new, part = pl.pallas_call(
            functools.partial(kernel, n),
            out_shape=(jax.ShapeDtypeStruct((d, wide), BF16),
                       jax.ShapeDtypeStruct((2, wide // COLS), F32)),
            in_specs=[vmem] * 3,
            out_specs=(vmem, vmem),
            scratch_shapes=[
                pltpu.VMEM((2, d, wide), BF16),
                pltpu.VMEM((2, d, wide), BF16),
                pltpu.VMEM((2, tokens, wide), BF16),
                pltpu.VMEM((d, tokens), BF16),
                pltpu.VMEM((d, tokens), BF16),
                pltpu.VMEM((2, d, tokens), BF16),
                pltpu.VMEM((2, d, tokens), BF16),
                pltpu.VMEM((2, d, tokens), BF16),
                pltpu.VMEM((2, wide // COLS), F32),
                pltpu.SemaphoreType.DMA((2, kinds, most)),
                pltpu.SemaphoreType.DMA((2, 2)),
            ],
            compiler_params=pltpu.CompilerParams(
                collective_id=0, has_side_effects=True, vmem_limit_bytes=60 * 1024 * 1024),
        )(x, h, t)
        errors = lax.psum(jnp.sum(part, axis=1), ("blk", "mp")) / total
        return new[None], errors

    placed = (P("blk", None, "mp"),) * 3
    return jax.shard_map(
        on_device, mesh=mesh, in_specs=placed,
        out_specs=(P("blk", None, "mp"), P()), check_vma=False)
```

```python
import functools

import jax
import jax.numpy as jnp
from jax import lax
from jax.experimental import pallas as pl
from jax.experimental.pallas import tpu as pltpu
from jax.sharding import PartitionSpec as P

MESH = pl.DeviceIdType.MESH
CHUNKS = 8
COLS = 4
GROUP = 8
FINALS = 5
mix_third = 1.0 / 3.0
step_size = 0.1
F32 = jnp.float32
BF16 = jnp.bfloat16


def dot_nt(a, b):
    return lax.dot_general(a, b, (((1,), (1,)), ((), ())), preferred_element_type=F32)


def dot_nn(a, b):
    return lax.dot_general(a, b, (((1,), (0,)), ((), ())), preferred_element_type=F32)


def kernel(n, total, x, h, t, out, err, xo, far, near, hn, rt, rt2, rn, ps, pr, acc, red_a, red_b, sems, one, asem, bsem, osem):
    d, wide = x.shape
    tokens = h.shape[0]
    half = t.shape[1]
    rows = d // CHUNKS
    cw = wide // COLS
    zs = n // 4
    me = lax.axis_index("blk")
    mp = lax.axis_index("mp")
    core = lax.rem(me, 2)
    par = lax.rem(me // 2, 2)
    low = lax.rem(me, 4)
    z = me // 4
    spot = low * 2 + mp
    sib = me + 1 - 2 * core
    partner = me + 2 - 4 * par
    fwd_to = lax.rem(me + n + 4 - 8 * par, n)
    cross = lax.rem(me + n + 2 * core - 1, n)

    def in_group(o):
        there = lax.rem(spot + o, GROUP)
        return there, (z * 4 + there // 2, lax.rem(there, 2))

    def over_groups(o):
        there = lax.rem(z + o, zs)
        return there, (there * 4 + low, mp)

    barrier = pltpu.get_barrier_semaphore()
    for o in range(1, GROUP):
        pl.semaphore_signal(barrier, inc=1, device_id=in_group(o)[1], device_id_type=MESH)
    for o in range(1, zs):
        pl.semaphore_signal(barrier, inc=1, device_id=over_groups(o)[1], device_id_type=MESH)
    pl.semaphore_signal(barrier, inc=1, device_id=(cross, mp), device_id_type=MESH)
    pl.semaphore_wait(barrier, GROUP + zs - 1)

    def rs(k):
        return pl.ds(k * rows, rows)

    def remote(src, dst, send, recv, dev):
        return pltpu.make_async_remote_copy(
            src_ref=src, dst_ref=dst, send_sem=send, recv_sem=recv, device_id=dev, device_id_type=MESH)

    def copy(src, dst, kind, k, dev):
        return remote(src, dst, sems.at[0, kind, k], sems.at[1, kind, k], dev)

    def c_own(k):
        return copy(x.at[rs(k)], far.at[par, rs(k)], 0, k, (partner, mp))

    def c_fwd(k):
        return copy(far.at[1 - par, rs(k)], far.at[par, rs(k)], 1, k, (fwd_to, mp))

    def c_cross(k):
        return copy(far.at[1 - core, rs(k)], near.at[1 - core, rs(k)], 2, k, (sib, mp))

    def c_rsib(k):
        return copy(rt.at[rs(k)], rn.at[core, rs(k)], 3, k, (sib, mp))

    def mine(k):
        return pl.ds(pl.multiple_of(mp * half + k * rows, rows), rows)

    def c_rcross(k):
        return copy(rt.at[mine(k)], rn.at[1 - core, mine(k)], 4, k, (cross, mp))

    def c_rmp(k):
        return copy(rn.at[core, mine(k)], rn.at[core, mine(k)], 8, k, (me, 1 - mp))

    def c_part(it, k):
        return copy(ps.at[it, rs(k)], pr.at[it, rs(k)], 5 + it, k, (me, 1 - mp))

    def c_hcross(j):
        cs = pl.ds(j * cw, cw)
        return copy(h.at[:, cs], hn.at[1 - core, :, cs], 7, j, (cross, mp))

    def c_out(k):
        return pltpu.make_async_copy(xo.at[rs(k)], out.at[rs(k)], osem.at[k])

    def c_group(o):
        there, dev = in_group(o)
        return remote(red_a.at[spot], red_a.at[spot], asem.at[0, o], asem.at[1, spot], dev)

    def from_group(o):
        there, dev = in_group(o)
        return remote(red_a.at[there], red_a.at[there], asem.at[0, o], asem.at[1, there], dev)

    def c_over(o):
        there, dev = over_groups(o)
        return remote(red_b.at[z], red_b.at[z], bsem.at[0, o], bsem.at[1, z], dev)

    def from_over(o):
        there, dev = over_groups(o)
        return remote(red_b.at[there], red_b.at[there], bsem.at[0, o], bsem.at[1, there], dev)

    c_sib = remote(x, near.at[core], one.at[0, 0], one.at[1, 0], (sib, mp))
    c_hsib = remote(h, hn.at[core], one.at[0, 1], one.at[1, 1], (sib, mp))

    def send_part(it, k, value):
        first = k * rows
        here = mp == first // half
        targ = t[:, pl.ds(first % half, rows)].astype(F32).T
        ps[it, rs(k), :] = (value - jnp.where(here, targ, 0.0)).astype(BF16)
        c_part(it, k).start()

    def take_part(it, k, dst):
        c_part(it, k).wait_recv()
        dst[rs(k), :] = (ps[it, rs(k), :].astype(F32) + pr[it, rs(k), :].astype(F32)).astype(BF16)

    def add_err(row, diff):
        v = jnp.sum(diff * diff, axis=0, keepdims=True)
        acc[row:row + 1, :] += sum(v[:, q:q + 128] for q in range(0, cw, 128))

    def columns(j):
        return pl.ds(pl.multiple_of(j * cw, cw), cw)

    def neighbour(r, cs, side):
        track = (dot_nn(rn[side, r, :], hn[side, :, cs]) / tokens).astype(BF16).astype(F32)
        own, there, beyond = x[r, cs].astype(F32), near[side, r, cs].astype(F32), far[side, r, cs].astype(F32)
        state = (own + there + beyond) * mix_third - step_size * track
        return track, state.astype(BF16).astype(F32)

    def err_pass(k):
        def body(j, _):
            cs = columns(j)
            add_err(1, xo[rs(k), cs].astype(F32) - neighbour(rs(k), cs, 1)[1])
            return 0
        lax.fori_loop(0, COLS, body, 0)

    def last_step(k, with_err):
        r = rs(k)

        def body(j, _):
            cs = columns(j)
            older = dot_nn(rt[r, :], h[:, cs]) / tokens
            fresh = dot_nn(rt2[r, :], h[:, cs]) / tokens
            below, x_lo = neighbour(r, cs, 0)
            above, x_hi = neighbour(r, cs, 1)
            track = older.astype(BF16).astype(F32)
            track = ((below + track + above) * mix_third + fresh - older).astype(BF16).astype(F32)
            x_me = xo[r, cs].astype(F32)
            if with_err:
                add_err(1, x_me - x_hi)
            xo[r, cs] = ((x_lo + x_me + x_hi) * mix_third - step_size * track).astype(BF16)
            return 0

        lax.fori_loop(0, COLS, body, 0)
        c_out(k).start()

    def middle_step(k):
        def body(j, _):
            cs = columns(j)
            track = (dot_nn(rt[rs(k), :], h[:, cs]) / tokens).astype(BF16)
            own = x[rs(k), cs].astype(F32)
            above = near[1, rs(k), cs].astype(F32)
            add_err(0, own - above)
            blend = (near[0, rs(k), cs].astype(F32) + own + above) * mix_third
            xo[rs(k), cs] = (blend - step_size * track.astype(F32)).astype(BF16)
            return 0

        lax.fori_loop(0, COLS, body, 0)
        send_part(1, k, dot_nt(xo[rs(k), :], h[...]))

    early = 2
    halves = half // rows
    for k in range(early):
        c_own(k).start()
    c_sib.start()
    c_hsib.start()
    acc[...] = jnp.zeros_like(acc)
    for k in range(CHUNKS):
        send_part(0, k, dot_nt(x[rs(k), :], h[...]))
    for k in range(CHUNKS):
        take_part(0, k, rt)
    for k in range(halves):
        c_rcross(k).start()
    for k in range(CHUNKS):
        c_rsib(k).start()
    for j in range(COLS):
        c_hcross(j).start()
    c_sib.wait_recv()

    ready = FINALS
    done = 0
    for s in range(CHUNKS + 3):
        if s == ready:
            for k in range(halves):
                c_rcross(k).wait_recv()
                c_rmp(k).start()
            c_hsib.wait_recv()
            for k in range(CHUNKS):
                c_rsib(k).wait_recv()
            for j in range(COLS):
                c_hcross(j).wait_recv()
            for k in range(halves):
                c_rmp(k).wait_recv()
        if 0 <= s - 2 < CHUNKS:
            c_cross(s - 2).wait_recv()
            middle_step(s - 2)
        if 0 <= s - 1 < CHUNKS:
            c_fwd(s - 1).wait_recv()
            c_cross(s - 1).start()
        if s < CHUNKS:
            c_own(s).wait_recv()
            c_fwd(s).start()
            if s + early < CHUNKS:
                c_own(s + early).start()
        if s - 3 == CHUNKS - 1:
            err_pass(CHUNKS - 1)
            red_a[spot] = acc[...]
            for o in range(1, GROUP):
                c_group(o).start()
        if 0 <= s - 3 < CHUNKS:
            take_part(1, s - 3, rt2)
        if s >= ready:
            for k in range(done, min(s - 2, done + 2, CHUNKS)):
                last_step(k, k < CHUNKS - 1)
                done = k + 1

    for k in range(done, CHUNKS):
        last_step(k, k < CHUNKS - 1)
    for o in range(1, GROUP):
        from_group(o).wait_recv()
    value = red_a[0]
    for o in range(1, GROUP):
        value += red_a[o]
    red_b[z] = value
    for o in range(1, zs):
        c_over(o).start()
    c_sib.wait_send()
    c_hsib.wait_send()
    for k in range(CHUNKS):
        for c in (c_own(k), c_fwd(k), c_cross(k), c_rsib(k), c_part(0, k), c_part(1, k)):
            c.wait_send()
        c_out(k).wait()
    for k in range(halves):
        c_rcross(k).wait_send()
        c_rmp(k).wait_send()
    for j in range(COLS):
        c_hcross(j).wait_send()
    for o in range(1, GROUP):
        c_group(o).wait_send()
    for o in range(1, zs):
        from_over(o).wait_recv()
    value = red_b[0]
    for o in range(1, zs):
        value += red_b[o]
    for o in range(1, zs):
        c_over(o).wait_send()
    for row in range(2):
        err[row] = jnp.sum(value[row:row + 1, :]) / total


def solution(mesh):
    n = mesh.shape["blk"]

    def on_device(params, hidden, targets):
        x, h, t = params[0], hidden[0], targets[0]
        d, wide = x.shape
        tokens = h.shape[0]
        total = float(wide * mesh.shape["mp"] * n)
        vmem = pl.BlockSpec(memory_space=pltpu.VMEM)
        dma = pltpu.SemaphoreType.DMA
        new, errors = pl.pallas_call(
            functools.partial(kernel, n, total),
            out_shape=(jax.ShapeDtypeStruct((d, wide), BF16), jax.ShapeDtypeStruct((2,), F32)),
            in_specs=[vmem] * 3,
            out_specs=(pl.BlockSpec(memory_space=pl.ANY), pl.BlockSpec(memory_space=pltpu.SMEM)),
            scratch_shapes=[
                pltpu.VMEM((d, wide), BF16),
                pltpu.VMEM((2, d, wide), BF16),
                pltpu.VMEM((2, d, wide), BF16),
                pltpu.VMEM((2, tokens, wide), BF16),
                pltpu.VMEM((d, tokens), BF16),
                pltpu.VMEM((d, tokens), BF16),
                pltpu.VMEM((2, d, tokens), BF16),
                pltpu.VMEM((2, d, tokens), BF16),
                pltpu.VMEM((2, d, tokens), BF16),
                pltpu.VMEM((8, 128), F32),
                pltpu.VMEM((GROUP, 8, 128), F32),
                pltpu.VMEM((n // 4, 8, 128), F32),
                dma((2, 9, max(CHUNKS, COLS))),
                dma((2, 2)),
                dma((2, GROUP)),
                dma((2, n // 4)),
                dma((CHUNKS,)),
            ],
            compiler_params=pltpu.CompilerParams(
                collective_id=0, has_side_effects=True, vmem_limit_bytes=60 * 1024 * 1024),
        )(x, h, t)
        return new[None], errors

    placed = (P("blk", None, "mp"),) * 3
    return jax.shard_map(
        on_device, mesh=mesh, in_specs=placed,
        out_specs=(P("blk", None, "mp"), P()), check_vma=False)
```

```python
import functools

import jax
import jax.numpy as jnp
from jax import lax
from jax.experimental import pallas as pl
from jax.experimental.pallas import tpu as pltpu
from jax.sharding import PartitionSpec as P

MESH = pl.DeviceIdType.MESH
PARTS = 8
SIZES = (2, 2, 2, 2, 2, 2, 1, 1, 1, 1)
CHUNKS = len(SIZES)
COLS = 4
GROUP = 8
FINALS = 5
mix_third = 1.0 / 3.0
step_size = 0.1
F32 = jnp.float32
BF16 = jnp.bfloat16


def dot_nt(a, b):
    return lax.dot_general(a, b, (((1,), (1,)), ((), ())), preferred_element_type=F32)


def dot_nn(a, b):
    return lax.dot_general(a, b, (((1,), (0,)), ((), ())), preferred_element_type=F32)


def kernel(n, total, x, h, t, xo, err, far, near, hn, rt, rt2, rn, ps, pr, acc, red_a, red_b, sems, one, asem, bsem):
    d, wide = x.shape
    tokens = h.shape[0]
    half = t.shape[1]
    rows = d // PARTS
    unit = d // sum(SIZES)
    cw = wide // COLS
    zs = n // 4
    me = lax.axis_index("blk")
    mp = lax.axis_index("mp")
    core = lax.rem(me, 2)
    par = lax.rem(me // 2, 2)
    low = lax.rem(me, 4)
    z = me // 4
    spot = low * 2 + mp
    sib = me + 1 - 2 * core
    partner = me + 2 - 4 * par
    fwd_to = lax.rem(me + n + 4 - 8 * par, n)
    cross = lax.rem(me + n + 2 * core - 1, n)

    def in_group(o):
        there = lax.rem(spot + o, GROUP)
        return there, (z * 4 + there // 2, lax.rem(there, 2))

    def over_groups(o):
        there = lax.rem(z + o, zs)
        return there, (there * 4 + low, mp)

    barrier = pltpu.get_barrier_semaphore()
    for o in range(1, GROUP):
        pl.semaphore_signal(barrier, inc=1, device_id=in_group(o)[1], device_id_type=MESH)
    for o in range(1, zs):
        pl.semaphore_signal(barrier, inc=1, device_id=over_groups(o)[1], device_id_type=MESH)
    pl.semaphore_signal(barrier, inc=1, device_id=(cross, mp), device_id_type=MESH)
    pl.semaphore_wait(barrier, GROUP + zs - 1)

    def rs(k):
        return pl.ds(sum(SIZES[:k]) * unit, SIZES[k] * unit)

    def remote(src, dst, send, recv, dev):
        return pltpu.make_async_remote_copy(
            src_ref=src, dst_ref=dst, send_sem=send, recv_sem=recv, device_id=dev, device_id_type=MESH)

    def copy(src, dst, kind, k, dev):
        return remote(src, dst, sems.at[0, kind, k], sems.at[1, kind, k], dev)

    def c_own(k):
        return copy(x.at[rs(k)], far.at[par, rs(k)], 0, k, (partner, mp))

    def c_fwd(k):
        return copy(far.at[1 - par, rs(k)], far.at[par, rs(k)], 1, k, (fwd_to, mp))

    def c_cross(k):
        return copy(far.at[1 - core, rs(k)], near.at[1 - core, rs(k)], 2, k, (sib, mp))

    def c_rsib(k):
        return copy(rt.at[rs(k)], rn.at[core, rs(k)], 3, k, (sib, mp))

    def mine(k):
        return pl.ds(pl.multiple_of(mp * half + k * rows, rows), rows)

    def c_rcross(k):
        return copy(rt.at[mine(k)], rn.at[1 - core, mine(k)], 4, k, (cross, mp))

    def c_rmp(k):
        return copy(rn.at[core, mine(k)], rn.at[core, mine(k)], 8, k, (me, 1 - mp))

    def c_part(it, k):
        return copy(ps.at[it, rs(k)], pr.at[it, rs(k)], 5 + it, k, (me, 1 - mp))

    def c_hcross(j):
        cs = pl.ds(j * cw, cw)
        return copy(h.at[:, cs], hn.at[1 - core, :, cs], 7, j, (cross, mp))

    def c_group(o):
        there, dev = in_group(o)
        return remote(red_a.at[spot], red_a.at[spot], asem.at[0, o], asem.at[1, spot], dev)

    def from_group(o):
        there, dev = in_group(o)
        return remote(red_a.at[there], red_a.at[there], asem.at[0, o], asem.at[1, there], dev)

    def c_over(o):
        there, dev = over_groups(o)
        return remote(red_b.at[z], red_b.at[z], bsem.at[0, o], bsem.at[1, z], dev)

    def from_over(o):
        there, dev = over_groups(o)
        return remote(red_b.at[there], red_b.at[there], bsem.at[0, o], bsem.at[1, there], dev)

    c_sib = remote(x, near.at[core], one.at[0, 0], one.at[1, 0], (sib, mp))
    c_hsib = remote(h, hn.at[core], one.at[0, 1], one.at[1, 1], (sib, mp))

    def send_part(it, k, value):
        first = sum(SIZES[:k]) * unit
        here = mp == first // half
        targ = t[:, pl.ds(first % half, SIZES[k] * unit)].astype(F32).T
        ps[it, rs(k), :] = (value - jnp.where(here, targ, 0.0)).astype(BF16)
        c_part(it, k).start()

    def take_part(it, k, dst):
        c_part(it, k).wait_recv()
        dst[rs(k), :] = (ps[it, rs(k), :].astype(F32) + pr[it, rs(k), :].astype(F32)).astype(BF16)

    def add_err(row, diff):
        v = jnp.sum(diff * diff, axis=0, keepdims=True)
        acc[row:row + 1, :] += sum(v[:, q:q + 128] for q in range(0, cw, 128))

    def columns(j):
        return pl.ds(pl.multiple_of(j * cw, cw), cw)

    def neighbour(r, cs, side):
        track = (dot_nn(rn[side, r, :], hn[side, :, cs]) / tokens).astype(BF16).astype(F32)
        own, there, beyond = x[r, cs].astype(F32), near[side, r, cs].astype(F32), far[side, r, cs].astype(F32)
        state = (own + there + beyond) * mix_third - step_size * track
        return track, state.astype(BF16).astype(F32)

    def err_pass(k):
        def body(j, _):
            cs = columns(j)
            add_err(1, xo[rs(k), cs].astype(F32) - neighbour(rs(k), cs, 1)[1])
            return 0
        lax.fori_loop(0, COLS, body, 0)

    def last_step(k, with_err):
        r = rs(k)

        def body(j, _):
            cs = columns(j)
            older = dot_nn(rt[r, :], h[:, cs]) / tokens
            fresh = dot_nn(rt2[r, :], h[:, cs]) / tokens
            below, x_lo = neighbour(r, cs, 0)
            above, x_hi = neighbour(r, cs, 1)
            track = older.astype(BF16).astype(F32)
            track = ((below + track + above) * mix_third + fresh - older).astype(BF16).astype(F32)
            x_me = xo[r, cs].astype(F32)
            if with_err:
                add_err(1, x_me - x_hi)
            xo[r, cs] = ((x_lo + x_me + x_hi) * mix_third - step_size * track).astype(BF16)
            return 0

        lax.fori_loop(0, COLS, body, 0)

    def middle_step(k):
        def body(j, _):
            cs = columns(j)
            track = (dot_nn(rt[rs(k), :], h[:, cs]) / tokens).astype(BF16)
            own = x[rs(k), cs].astype(F32)
            above = near[1, rs(k), cs].astype(F32)
            add_err(0, own - above)
            blend = (near[0, rs(k), cs].astype(F32) + own + above) * mix_third
            xo[rs(k), cs] = (blend - step_size * track.astype(F32)).astype(BF16)
            return 0

        lax.fori_loop(0, COLS, body, 0)
        send_part(1, k, dot_nt(xo[rs(k), :], h[...]))

    early = 3
    last = CHUNKS - 1
    halves = half // rows
    for k in range(early):
        c_own(k).start()
    c_sib.start()
    c_hsib.start()
    acc[...] = jnp.zeros_like(acc)
    for k in range(CHUNKS):
        send_part(0, k, dot_nt(x[rs(k), :], h[...]))
    for k in range(CHUNKS):
        take_part(0, k, rt)
    for k in range(halves):
        c_rcross(k).start()
    for k in range(CHUNKS):
        c_rsib(k).start()
    for j in range(COLS):
        c_hcross(j).start()
    c_sib.wait_recv()

    ready = FINALS
    done = 0
    for s in range(CHUNKS + 3):
        if s == ready:
            for k in range(halves):
                c_rcross(k).wait_recv()
                c_rmp(k).start()
            c_hsib.wait_recv()
            for k in range(CHUNKS):
                c_rsib(k).wait_recv()
            for j in range(COLS):
                c_hcross(j).wait_recv()
            for k in range(halves):
                c_rmp(k).wait_recv()
        if s - 2 == last:
            err_pass(last - 1)
        if 0 <= s - 2 < CHUNKS:
            c_cross(s - 2).wait_recv()
            middle_step(s - 2)
        if 0 <= s - 1 < CHUNKS:
            c_fwd(s - 1).wait_recv()
            c_cross(s - 1).start()
        if s < CHUNKS:
            c_own(s).wait_recv()
            c_fwd(s).start()
            if s + early < CHUNKS:
                c_own(s + early).start()
        if s - 2 == last:
            err_pass(last)
            red_a[spot] = acc[...]
            for o in range(1, GROUP):
                c_group(o).start()
        if s - 3 == last:
            for o in range(1, GROUP):
                from_group(o).wait_recv()
            value = red_a[0]
            for o in range(1, GROUP):
                value += red_a[o]
            red_b[z] = value
            for o in range(1, zs):
                c_over(o).start()
        if 0 <= s - 3 < CHUNKS:
            take_part(1, s - 3, rt2)
        if s >= ready:
            for k in range(done, min(s - 2, done + 2, CHUNKS)):
                last_step(k, k < last - 1)
                done = k + 1

    c_sib.wait_send()
    c_hsib.wait_send()
    for k in range(CHUNKS):
        for c in (c_own(k), c_fwd(k), c_cross(k), c_rsib(k), c_part(0, k), c_part(1, k)):
            c.wait_send()
    for k in range(halves):
        c_rcross(k).wait_send()
        c_rmp(k).wait_send()
    for j in range(COLS):
        c_hcross(j).wait_send()
    for o in range(1, GROUP):
        c_group(o).wait_send()
    for o in range(1, zs):
        from_over(o).wait_recv()
    value = red_b[0]
    for o in range(1, zs):
        value += red_b[o]
    for o in range(1, zs):
        c_over(o).wait_send()
    for row in range(2):
        err[row] = jnp.sum(value[row:row + 1, :]) / total


def solution(mesh):
    n = mesh.shape["blk"]

    def on_device(params, hidden, targets):
        x, h, t = params[0], hidden[0], targets[0]
        d, wide = x.shape
        tokens = h.shape[0]
        total = float(wide * mesh.shape["mp"] * n)
        vmem = pl.BlockSpec(memory_space=pltpu.VMEM)
        dma = pltpu.SemaphoreType.DMA
        new, errors = pl.pallas_call(
            functools.partial(kernel, n, total),
            out_shape=(pltpu.VMEM((d, wide), BF16), jax.ShapeDtypeStruct((2,), F32)),
            in_specs=[vmem] * 3,
            out_specs=(vmem, pl.BlockSpec(memory_space=pltpu.SMEM)),
            scratch_shapes=[
                pltpu.VMEM((2, d, wide), BF16),
                pltpu.VMEM((2, d, wide), BF16),
                pltpu.VMEM((2, tokens, wide), BF16),
                pltpu.VMEM((d, tokens), BF16),
                pltpu.VMEM((d, tokens), BF16),
                pltpu.VMEM((2, d, tokens), BF16),
                pltpu.VMEM((2, d, tokens), BF16),
                pltpu.VMEM((2, d, tokens), BF16),
                pltpu.VMEM((8, 128), F32),
                pltpu.VMEM((GROUP, 8, 128), F32),
                pltpu.VMEM((n // 4, 8, 128), F32),
                dma((2, 9, max(CHUNKS, COLS))),
                dma((2, 2)),
                dma((2, GROUP)),
                dma((2, n // 4)),
            ],
            compiler_params=pltpu.CompilerParams(
                collective_id=0, has_side_effects=True, vmem_limit_bytes=48 * 1024 * 1024),
        )(x, h, t)
        return new[None], errors

    placed = (P("blk", None, "mp"),) * 3
    return jax.shard_map(
        on_device, mesh=mesh, in_specs=placed,
        out_specs=(P("blk", None, "mp"), P()), check_vma=False)
```

```python
import functools

import jax
import jax.numpy as jnp
from jax import lax
from jax.experimental import pallas as pl
from jax.experimental.pallas import tpu as pltpu
from jax.sharding import PartitionSpec as P

MESH = pl.DeviceIdType.MESH
PARTS = 8
SIZES = (2,) * 8
CHUNKS = len(SIZES)
COLS = 4
GROUP = 8
FINALS = 5
mix_third = 1.0 / 3.0
step_size = 0.1
F32 = jnp.float32
BF16 = jnp.bfloat16


def dot_nt(a, b):
    return lax.dot_general(a, b, (((1,), (1,)), ((), ())), preferred_element_type=F32)


def dot_nn(a, b):
    return lax.dot_general(a, b, (((1,), (0,)), ((), ())), preferred_element_type=F32)


def kernel(n, total, x, h, t, xo, err, far, near, hn, rt, rt2, rn, ps, pr, acc, red_a, red_b, sems, one, asem, bsem):
    d, wide = x.shape
    tokens = h.shape[0]
    half = t.shape[1]
    rows = d // PARTS
    unit = d // sum(SIZES)
    cw = wide // COLS
    zs = n // 4
    me = lax.axis_index("blk")
    mp = lax.axis_index("mp")
    core = lax.rem(me, 2)
    par = lax.rem(me // 2, 2)
    low = lax.rem(me, 4)
    z = me // 4
    spot = low * 2 + mp
    sib = me + 1 - 2 * core
    partner = me + 2 - 4 * par
    fwd_to = lax.rem(me + n + 4 - 8 * par, n)
    cross = lax.rem(me + n + 2 * core - 1, n)

    def in_group(o):
        there = lax.rem(spot + o, GROUP)
        return there, (z * 4 + there // 2, lax.rem(there, 2))

    def over_groups(o):
        there = lax.rem(z + o, zs)
        return there, (there * 4 + low, mp)

    barrier = pltpu.get_barrier_semaphore()
    for o in range(1, GROUP):
        pl.semaphore_signal(barrier, inc=1, device_id=in_group(o)[1], device_id_type=MESH)
    for o in range(1, zs):
        pl.semaphore_signal(barrier, inc=1, device_id=over_groups(o)[1], device_id_type=MESH)
    pl.semaphore_signal(barrier, inc=1, device_id=(cross, mp), device_id_type=MESH)
    pl.semaphore_wait(barrier, GROUP + zs - 1)

    def rs(k):
        return pl.ds(sum(SIZES[:k]) * unit, SIZES[k] * unit)

    def remote(src, dst, send, recv, dev):
        return pltpu.make_async_remote_copy(
            src_ref=src, dst_ref=dst, send_sem=send, recv_sem=recv, device_id=dev, device_id_type=MESH)

    def copy(src, dst, kind, k, dev):
        return remote(src, dst, sems.at[0, kind, k], sems.at[1, kind, k], dev)

    def c_own(k):
        return copy(x.at[rs(k)], far.at[par, rs(k)], 0, k, (partner, mp))

    def c_fwd(k):
        return copy(far.at[1 - par, rs(k)], far.at[par, rs(k)], 1, k, (fwd_to, mp))

    def c_cross(k):
        return copy(far.at[1 - core, rs(k)], near.at[1 - core, rs(k)], 2, k, (sib, mp))

    def c_rsib(k):
        return copy(rt.at[rs(k)], rn.at[core, rs(k)], 3, k, (sib, mp))

    def mine(k):
        return pl.ds(pl.multiple_of(mp * half + k * rows, rows), rows)

    def c_rcross(k):
        return copy(rt.at[mine(k)], rn.at[1 - core, mine(k)], 4, k, (cross, mp))

    def c_rmp(k):
        return copy(rn.at[core, mine(k)], rn.at[core, mine(k)], 8, k, (me, 1 - mp))

    def c_part(it, k):
        return copy(ps.at[it, rs(k)], pr.at[it, rs(k)], 5 + it, k, (me, 1 - mp))

    def c_hcross(j):
        cs = pl.ds(j * cw, cw)
        return copy(h.at[:, cs], hn.at[1 - core, :, cs], 7, j, (cross, mp))

    def c_group(o):
        there, dev = in_group(o)
        return remote(red_a.at[spot], red_a.at[spot], asem.at[0, o], asem.at[1, spot], dev)

    def from_group(o):
        there, dev = in_group(o)
        return remote(red_a.at[there], red_a.at[there], asem.at[0, o], asem.at[1, there], dev)

    def c_over(o):
        there, dev = over_groups(o)
        return remote(red_b.at[z], red_b.at[z], bsem.at[0, o], bsem.at[1, z], dev)

    def from_over(o):
        there, dev = over_groups(o)
        return remote(red_b.at[there], red_b.at[there], bsem.at[0, o], bsem.at[1, there], dev)

    c_sib = remote(x, near.at[core], one.at[0, 0], one.at[1, 0], (sib, mp))
    c_hsib = remote(h, hn.at[core], one.at[0, 1], one.at[1, 1], (sib, mp))

    def send_part(it, k, value):
        first = sum(SIZES[:k]) * unit
        here = mp == first // half
        targ = t[:, pl.ds(first % half, SIZES[k] * unit)].astype(F32).T
        ps[it, rs(k), :] = (value - jnp.where(here, targ, 0.0)).astype(BF16)
        c_part(it, k).start()

    def take_part(it, k, dst):
        c_part(it, k).wait_recv()
        dst[rs(k), :] = (ps[it, rs(k), :].astype(F32) + pr[it, rs(k), :].astype(F32)).astype(BF16)

    def add_err(row, diff):
        v = jnp.sum(diff * diff, axis=0, keepdims=True)
        acc[row:row + 1, :] += sum(v[:, q:q + 128] for q in range(0, cw, 128))

    def columns(j):
        return pl.ds(pl.multiple_of(j * cw, cw), cw)

    def neighbour(r, cs, side):
        track = (dot_nn(rn[side, r, :], hn[side, :, cs]) / tokens).astype(BF16).astype(F32)
        own, there, beyond = x[r, cs].astype(F32), near[side, r, cs].astype(F32), far[side, r, cs].astype(F32)
        state = (own + there + beyond) * mix_third - step_size * track
        return track, state.astype(BF16).astype(F32)

    def err_pass(k):
        def body(j, _):
            cs = columns(j)
            add_err(1, xo[rs(k), cs].astype(F32) - neighbour(rs(k), cs, 1)[1])
            return 0
        lax.fori_loop(0, COLS, body, 0)

    def last_step(k, with_err):
        r = rs(k)

        def body(j, _):
            cs = columns(j)
            older = dot_nn(rt[r, :], h[:, cs]) / tokens
            fresh = dot_nn(rt2[r, :], h[:, cs]) / tokens
            below, x_lo = neighbour(r, cs, 0)
            above, x_hi = neighbour(r, cs, 1)
            track = older.astype(BF16).astype(F32)
            track = ((below + track + above) * mix_third + fresh - older).astype(BF16).astype(F32)
            x_me = xo[r, cs].astype(F32)
            if with_err:
                add_err(1, x_me - x_hi)
            xo[r, cs] = ((x_lo + x_me + x_hi) * mix_third - step_size * track).astype(BF16)
            return 0

        lax.fori_loop(0, COLS, body, 0)

    def middle_step(k):
        def body(j, _):
            cs = columns(j)
            track = (dot_nn(rt[rs(k), :], h[:, cs]) / tokens).astype(BF16)
            own = x[rs(k), cs].astype(F32)
            above = near[1, rs(k), cs].astype(F32)
            add_err(0, own - above)
            blend = (near[0, rs(k), cs].astype(F32) + own + above) * mix_third
            xo[rs(k), cs] = (blend - step_size * track.astype(F32)).astype(BF16)
            return 0

        lax.fori_loop(0, COLS, body, 0)
        send_part(1, k, dot_nt(xo[rs(k), :], h[...]))

    early = 2
    last = CHUNKS - 1
    halves = half // rows
    for k in range(early):
        c_own(k).start()
    c_sib.start()
    c_hsib.start()
    acc[...] = jnp.zeros_like(acc)
    for k in range(CHUNKS):
        send_part(0, k, dot_nt(x[rs(k), :], h[...]))
    for k in range(CHUNKS):
        take_part(0, k, rt)
    for k in range(halves):
        c_rcross(k).start()
    for k in range(CHUNKS):
        c_rsib(k).start()
    for j in range(COLS):
        c_hcross(j).start()
    c_sib.wait_recv()

    ready = FINALS
    done = 0
    for s in range(CHUNKS + 3):
        if s == ready:
            for k in range(halves):
                c_rcross(k).wait_recv()
                c_rmp(k).start()
            c_hsib.wait_recv()
            for k in range(CHUNKS):
                c_rsib(k).wait_recv()
            for j in range(COLS):
                c_hcross(j).wait_recv()
            for k in range(halves):
                c_rmp(k).wait_recv()
        if s - 2 == last:
            err_pass(last - 1)
        if 0 <= s - 2 < CHUNKS:
            c_cross(s - 2).wait_recv()
            middle_step(s - 2)
        if 0 <= s - 1 < CHUNKS:
            c_fwd(s - 1).wait_recv()
            c_cross(s - 1).start()
        if s < CHUNKS:
            c_own(s).wait_recv()
            c_fwd(s).start()
            if s + early < CHUNKS:
                c_own(s + early).start()
        if s - 2 == last:
            err_pass(last)
            red_a[spot] = acc[...]
            for o in range(1, GROUP):
                c_group(o).start()
        if s - 3 == last:
            for o in range(1, GROUP):
                from_group(o).wait_recv()
            value = red_a[0]
            for o in range(1, GROUP):
                value += red_a[o]
            red_b[z] = value
            for o in range(1, zs):
                c_over(o).start()
        if 0 <= s - 3 < CHUNKS:
            take_part(1, s - 3, rt2)
        if s >= ready:
            for k in range(done, min(s - 2, done + 2, CHUNKS)):
                last_step(k, k < last - 1)
                done = k + 1

    c_sib.wait_send()
    c_hsib.wait_send()
    for k in range(CHUNKS):
        for c in (c_own(k), c_fwd(k), c_cross(k), c_rsib(k), c_part(0, k), c_part(1, k)):
            c.wait_send()
    for k in range(halves):
        c_rcross(k).wait_send()
        c_rmp(k).wait_send()
    for j in range(COLS):
        c_hcross(j).wait_send()
    for o in range(1, GROUP):
        c_group(o).wait_send()
    for o in range(1, zs):
        from_over(o).wait_recv()
    value = red_b[0]
    for o in range(1, zs):
        value += red_b[o]
    for o in range(1, zs):
        c_over(o).wait_send()
    for row in range(2):
        err[row] = jnp.sum(value[row:row + 1, :]) / total


def solution(mesh):
    n = mesh.shape["blk"]

    def on_device(params, hidden, targets):
        x, h, t = params[0], hidden[0], targets[0]
        d, wide = x.shape
        tokens = h.shape[0]
        total = float(wide * mesh.shape["mp"] * n)
        vmem = pl.BlockSpec(memory_space=pltpu.VMEM)
        dma = pltpu.SemaphoreType.DMA
        new, errors = pl.pallas_call(
            functools.partial(kernel, n, total),
            out_shape=(pltpu.VMEM((d, wide), BF16), jax.ShapeDtypeStruct((2,), F32)),
            in_specs=[vmem] * 3,
            out_specs=(vmem, pl.BlockSpec(memory_space=pltpu.SMEM)),
            scratch_shapes=[
                pltpu.VMEM((2, d, wide), BF16),
                pltpu.VMEM((2, d, wide), BF16),
                pltpu.VMEM((2, tokens, wide), BF16),
                pltpu.VMEM((d, tokens), BF16),
                pltpu.VMEM((d, tokens), BF16),
                pltpu.VMEM((2, d, tokens), BF16),
                pltpu.VMEM((2, d, tokens), BF16),
                pltpu.VMEM((2, d, tokens), BF16),
                pltpu.VMEM((8, 128), F32),
                pltpu.VMEM((GROUP, 8, 128), F32),
                pltpu.VMEM((n // 4, 8, 128), F32),
                dma((2, 9, max(CHUNKS, COLS))),
                dma((2, 2)),
                dma((2, GROUP)),
                dma((2, n // 4)),
            ],
            compiler_params=pltpu.CompilerParams(
                collective_id=0, has_side_effects=True, vmem_limit_bytes=48 * 1024 * 1024),
        )(x, h, t)
        return new[None], errors

    placed = (P("blk", None, "mp"),) * 3
    return jax.shard_map(
        on_device, mesh=mesh, in_specs=placed,
        out_specs=(P("blk", None, "mp"), P()), check_vma=False)
```
